32 devices in a mesh: parts: 2 (over y), mem: 4 (over z), space: 4 (over x, core).
Axes of the slice: x: 2, y: 2, z: 4, core: 2. Of those that a mesh axis runs over, the one named last changes fastest.
Arguments:
- ensemble: bfloat16 [64, 70, 8192], P('mem', None, ('parts', 'space')), parts along dimension 2, may hold values from -6 to 6
- transform: bfloat16 [128, 64], P('parts'), parts along dimension 0, may hold values from -0.75 to 0.75
- obs_operator: bfloat16 [16, 70], replicated, may hold values from -0.75 to 0.75
- obs_weight: float32 [16, 8192], P(None, ('parts', 'space')), parts along dimension 1, may hold values from 0.25 to 40, as said below
Outputs:
- analysis: bfloat16 [64, 70, 8192], P('mem', None, ('parts', 'space')), parts along dimension 2
- prior_gram: float32 [128, 64], P('parts'), parts along dimension 0
- posterior_gram: float32 [128, 64], P('parts'), parts along dimension 0
The draws below stay inside these ranges and needn't reach their ends.
There are 2 independent parts, one for each index of `parts`. The reference program is written for one: setup_inputs(seed, part) draws one part's arguments, and reference() takes and returns one part's arrays. A program takes and returns all parts, laid end to end along the dimension named above; an argument that names none is the same for every part. Nothing has to cross between parts.
Inputs may be any that keep to these rules, and one draw needn't show every extreme that they name: `obs_weight`: positive.
All inputs are finite; a program needn't handle non-finite values.
Results may differ from the reference program's by a relative error of at most 0.001.
Values may be sent and summed in bfloat16 or wider, within the bound.
A program may use at most 64 MiB of HBM per device.

```python
import math
import jax
import jax.numpy as jnp
from jax import lax

MEMBERS = 64
VARS = 70
OBS = 16
CELLS = 4096


def draw_obs_weight(key, part):
    first_key = jax.random.fold_in(jax.random.fold_in(key, 11), 0)
    levels = jax.random.uniform(first_key, (OBS, CELLS), jnp.float32)
    position = jnp.arange(CELLS, dtype=jnp.float32) / max(CELLS - 1, 1)
    ramp = 1.0 + 2.0 * position
    return 0.5 * jnp.exp(levels * math.log(10.0)) * ramp[None, :]


def level_of(rng, shape, cuts, low, top_value):
    level = 1.0
    for dim, shards_of in cuts:
        steps = jax.random.uniform(jax.random.fold_in(jax.random.fold_in(rng, 6), dim), (shards_of,), jnp.float32, low / len(cuts), top_value / len(cuts))
        level = level * jnp.repeat(jnp.exp(steps), shape[dim] // shards_of).reshape((-1,) + (1,) * (len(shape) - 1 - dim))
    return level


def bell_draw(rng, shape, deviation, reach, shards=(), held_as=jnp.bfloat16):
    array = deviation * jax.random.normal(rng, shape, jnp.float32)
    if shards:
        array = array * level_of(rng, shape, shards, -0.22, 0.18)
    return jnp.clip(array, -reach, reach).astype(held_as)


def setup_inputs(seed: int = 0, part: int = 0) -> dict:
    seeds = jax.random.split(jax.random.key(seed), 5)
    part_splits = jax.random.split(jax.random.fold_in(seeds[4], part), 5)
    ensemble = bell_draw(part_splits[0], (MEMBERS, VARS, CELLS), 1.0, 6.0, ((0, 4), (2, 4)))
    transform = bell_draw(part_splits[1], (MEMBERS, MEMBERS), MEMBERS ** -0.5, 0.75)
    obs_operator = bell_draw(seeds[2], (OBS, VARS), VARS ** -0.5, 0.75)
    obs_weight = draw_obs_weight(jax.random.fold_in(jax.random.fold_in(seeds[4], part), 71), part)
    return dict(ensemble=ensemble, transform=transform, obs_operator=obs_operator, obs_weight=obs_weight)


def reference(ensemble, transform, obs_operator, obs_weight):
    mixing = transform.astype(jnp.float32)
    members = ensemble.astype(jnp.float32)
    member_mean = jnp.sum(members, axis=0) / MEMBERS
    combined = jnp.einsum("ij,ivc->jvc", mixing, members)
    keep_mean = 1.0 - jnp.sum(mixing, axis=0)
    analysis = (combined + member_mean[None, :, :] * keep_mean[:, None, None]).astype(jnp.bfloat16)
    observed = jnp.einsum("ov,mvc->moc", obs_operator.astype(jnp.float32), members)
    departures = observed - jnp.sum(observed, axis=0) / MEMBERS
    weighted = departures * obs_weight[None, :, :]
    gram_sum = jnp.einsum("ioc,joc->ij", weighted, departures, precision=lax.Precision.HIGHEST)
    prior_gram = gram_sum / jnp.sum(obs_weight)
    carried = jnp.dot(mixing.T, prior_gram, precision=lax.Precision.HIGHEST)
    posterior_gram = jnp.dot(carried, mixing, precision=lax.Precision.HIGHEST)
    return analysis, prior_gram, posterior_gram
```

```python
import functools

import jax
import jax.numpy as jnp
from jax import lax
from jax.experimental import pallas as pl
from jax.experimental.pallas import tpu as pltpu
from jax.sharding import PartitionSpec as P

HIGHEST = lax.Precision.HIGHEST
MESH = pl.DeviceIdType.MESH
LANES = 128
PIECE = 14
ROWS = 16
LEAD = 2
NT = (((1,), (1,)), ((), ()))


def dot(a, b):
    return jnp.dot(a, b, preferred_element_type=jnp.float32)


def selector(shape, match):
    rows = lax.broadcasted_iota(jnp.int32, shape, 0)
    cols = lax.broadcasted_iota(jnp.int32, shape, 1)
    return match(rows, cols)


def as_bf16(mask):
    return jnp.where(mask, 1.0, 0.0).astype(jnp.bfloat16)


def peers_of(me, size):
    if size % 2:
        return [lax.rem(me + step, size) for step in range(1, size)], []
    half = size // 2
    side, place = me // half, lax.rem(me, half)
    across = [(1 - side) * half + lax.rem(place + step, half) for step in range(half)]
    return across, [side * half + lax.rem(place + step, half) for step in range(1, half)]


def when(needed, condition, body):
    if needed:
        pl.when(condition)(body)
    else:
        body()


def line_kernel(
    sizes, ensemble, *refs,
):
    smalls, refs = refs[:3], refs[3:]
    analysis, prior, posterior, transform, obs_operator, obs_weight, small_sem = refs[:7]
    (
    arrived, results, observer, observed, gram, by_space, by_mem, in_slabs, out_slabs,
    in_send, in_recv, out_send, out_recv, own_in, own_out,
    space_send, space_recv, mem_send, mem_recv,
    ) = refs[7:]
    n_mem, n_space, active, pieces, local, members, variables, n_obs, chunk = sizes
    blocks = members // ROWS
    aligned = local % ROWS == 0
    partial_owners = active < n_mem
    me = lax.axis_index("mem")
    here = lax.axis_index("space")
    across, beside = peers_of(me, n_mem)
    mem_peers = across + beside
    space_peers = sum(peers_of(here, n_space), [])
    central = jnp.logical_or(me * 2 == n_mem, (me + 1) * 2 == n_mem)

    def lanes_of(owner):
        return pl.ds(pl.multiple_of(owner * chunk, chunk), chunk)

    def rows_of(device):
        return pl.ds(pl.multiple_of(device * local, local), local)

    barrier = pltpu.get_barrier_semaphore()
    for peer in mem_peers:
        pl.semaphore_signal(barrier, inc=1, device_id={"mem": peer}, device_id_type=MESH)
    for peer in space_peers:
        pl.semaphore_signal(barrier, inc=1, device_id={"space": peer}, device_id_type=MESH)
    pl.semaphore_wait(barrier, n_mem - 1 + n_space - 1)

    def spot(whole, slabs, piece, device):
        start, count = pieces[piece]
        if aligned:
            return whole.at[start : start + count, rows_of(device), :]
        return slabs.at[device, start : start + count]

    def outside(array, piece, owner):
        start, count = pieces[piece]
        return array.at[start : start + count, :, lanes_of(owner)]

    def inward(piece, peer, source):
        return pltpu.make_async_remote_copy(
            src_ref=outside(ensemble, piece, peer),
            dst_ref=spot(arrived, in_slabs, piece, source),
            send_sem=in_send.at[piece, peer],
            recv_sem=in_recv.at[piece, source],
            device_id={"mem": peer},
            device_id_type=MESH,
        )

    def inward_own(piece):
        return pltpu.make_async_copy(
            outside(ensemble, piece, me), spot(arrived, in_slabs, piece, me), own_in.at[piece]
        )

    def outward(piece, peer, owner):
        return pltpu.make_async_remote_copy(
            src_ref=spot(results, out_slabs, piece, peer),
            dst_ref=outside(analysis, piece, owner),
            send_sem=out_send.at[piece, peer],
            recv_sem=out_recv.at[piece, owner],
            device_id={"mem": peer},
            device_id_type=MESH,
        )

    def outward_own(piece):
        return pltpu.make_async_copy(
            spot(results, out_slabs, piece, me), outside(analysis, piece, me), own_out.at[piece]
        )

    owns = me < active
    for group in (beside, across):
        for piece in range(len(pieces)):
            for peer in group:
                when(partial_owners, peer < active, lambda: inward(piece, peer, me).start())
    for piece in range(len(pieces)):
        when(partial_owners, owns, lambda: inward_own(piece).start())
    loads = [
        pltpu.make_async_copy(source, target, small_sem.at[index])
        for index, (source, target) in enumerate(
            zip(smalls, (transform, obs_operator, obs_weight))
        )
    ]
    for load in loads:
        load.start()
    for load in loads:
        load.wait()

    eye = as_bf16(selector((members, members), lambda r, c: r == c))
    mixing_t = lax.dot_general(eye, transform[...], NT, preferred_element_type=jnp.float32)
    keep = 1.0 - jnp.sum(mixing_t, axis=1, keepdims=True)
    ones = jnp.ones((ROWS, members), jnp.float32)
    mixer = jnp.concatenate([mixing_t, ones], axis=0).astype(jnp.bfloat16)

    obs_rows = n_obs * ROWS
    obs_pick = as_bf16(selector((obs_rows, n_obs), lambda r, c: r // ROWS == c))
    for piece, (start, count) in enumerate(pieces):
        depth = count * ROWS
        place = as_bf16(selector((variables, depth), lambda r, c: r == c // ROWS + start))
        part = dot(obs_operator[...], place).astype(jnp.bfloat16)
        mask = selector((obs_rows, depth), lambda r, c: lax.rem(r, ROWS) == lax.rem(c, ROWS))
        full = jnp.where(mask, dot(obs_pick, part), 0.0)
        observer[piece, :, 0:depth] = full.astype(jnp.bfloat16)

    def mix(piece):
        start, count = pieces[piece]
        for variable in range(start, start + count):
            if not aligned:
                for device in range(n_mem):
                    rows = slice(device * local, (device + 1) * local)
                    arrived[variable, rows, :] = in_slabs[device, variable]
            mixed = dot(mixer, arrived[variable])
            mean = mixed[members : members + 1, :] / members
            value = (mixed[:members, :] + keep * mean).astype(jnp.bfloat16)
            if aligned:
                results[variable] = value
            else:
                for device in range(n_mem):
                    rows = slice(device * local, (device + 1) * local)
                    out_slabs[device, variable] = value[rows, :]

    def observe(piece):
        start, count = pieces[piece]
        depth = count * ROWS
        for block in range(blocks):
            at = slice(block * ROWS, (block + 1) * ROWS)
            states = arrived[start : start + count, at, :].reshape(depth, chunk)
            term = dot(observer[piece, :, 0:depth], states).reshape(n_obs, ROWS, chunk)
            if piece == 0:
                observed[:, at, :] = term
            else:
                observed[:, at, :] += term

    def form_gram():
        weights = obs_weight[:, lanes_of(me)]
        total = jnp.zeros((members, members), jnp.float32)
        for quantity in range(n_obs):
            values = observed[quantity]
            departures = values - jnp.sum(values, axis=0, keepdims=True) / members
            total += lax.dot_general(
                departures * weights[quantity : quantity + 1, :],
                departures,
                NT,
                precision=HIGHEST,
                preferred_element_type=jnp.float32,
            )
        gram[0:members, 0:members] = total
        gram[members : members + 8, :] = jnp.full((8, LANES), jnp.sum(weights), jnp.float32)

    gram[...] = jnp.zeros_like(gram)

    last = len(pieces) - 1

    def send_back(piece, group):
        for peer in group:
            outward(piece, peer, me).start()

    def work():
        for piece in range(last + 1):
            for peer in mem_peers:
                inward(piece, me, peer).wait_recv()
            inward_own(piece).wait()
            mix(piece)
            send_back(piece, beside)
            if piece < last:
                pl.when(central)(lambda: send_back(piece, across))
            outward_own(piece).start()
            observe(piece)
        form_gram()

    def finish_sends():
        for piece in range(last):
            pl.when(jnp.logical_not(central))(lambda: send_back(piece, across))
        send_back(last, across)

    when(partial_owners, owns, work)

    def exchange(source, slots, index, peers, axis, send, recv, between):
        slots[index] = source
        copies = [
            pltpu.make_async_remote_copy(
                src_ref=slots.at[index],
                dst_ref=slots.at[index],
                send_sem=send.at[peer],
                recv_sem=recv.at[index],
                device_id={axis: peer},
                device_id_type=MESH,
            )
            for peer in peers
        ]
        for copy in copies:
            copy.start()
        between()
        for peer in peers:
            pltpu.make_async_remote_copy(
                src_ref=slots.at[peer],
                dst_ref=slots.at[peer],
                send_sem=send.at[peer],
                recv_sem=recv.at[peer],
                device_id={axis: peer},
                device_id_type=MESH,
            ).wait_recv()
        total = slots[0]
        for slot in range(1, slots.shape[0]):
            total += slots[slot]
        for copy in copies:
            copy.wait_send()
        return total

    total = exchange(
        gram[...], by_space, here, space_peers, "space", space_send, space_recv, lambda: None
    )
    total = exchange(
        total, by_mem, me, mem_peers, "mem", mem_send, mem_recv,
        lambda: when(partial_owners, owns, finish_sends),
    )
    prior_gram = total[0:members, 0:members] / total[members : members + 1, 0:members]
    prior[...] = prior_gram
    carried = jnp.dot(
        mixing_t, prior_gram, precision=HIGHEST, preferred_element_type=jnp.float32
    )
    posterior[...] = jnp.dot(
        carried,
        transform[...].astype(jnp.float32),
        precision=HIGHEST,
        preferred_element_type=jnp.float32,
    )

    for piece in range(len(pieces)):
        for peer in mem_peers:
            when(partial_owners, peer < active, lambda: inward(piece, peer, me).wait_send())
            when(partial_owners, owns, lambda: outward(piece, peer, me).wait_send())
            when(partial_owners, peer < active, lambda: outward(piece, me, peer).wait_recv())
        when(partial_owners, owns, lambda: outward_own(piece).wait())


def hub_kernel(
    sizes, ensemble, transform_in, operator_in, weight_in, analysis, prior, posterior,
    transform, obs_operator, obs_weight, small_sem,
    arrived, relay, results, observer, observed, gram, parts, summed, crossed, totals,
    own_in, end_send, end_recv, relay_send, relay_recv, raw_send, raw_recv,
    forward_send, forward_recv, beside_send, far_send, near_send, out_recv, near_recv,
    part_send, part_recv, cross_send, cross_recv, total_send, total_recv, last_send, last_recv,
    met, ready,
):
    n_mem, n_space, pieces, local, members, variables, n_obs, half = sizes
    blocks = members // ROWS
    quarter = members // n_space
    me = lax.axis_index("mem")
    here = lax.axis_index("space")
    side = me // (n_mem // 2)
    is_hub = jnp.logical_or(me * 2 == n_mem, (me + 1) * 2 == n_mem)
    is_end = jnp.logical_not(is_hub)
    last_mem = n_mem - 1
    own_hub, far_hub = 1 + side, 2 - side
    own_end, far_end = last_mem * side, last_mem - last_mem * side
    space_peers = [lax.rem(here + step, n_space) for step in range(1, n_space)]
    order = range(len(pieces))

    def lanes_of(which):
        return pl.ds(pl.multiple_of(which * half, half), half)

    def rows_of(device):
        return pl.ds(pl.multiple_of(device * local, local), local)

    def quarter_of(device):
        return pl.ds(pl.multiple_of(device * quarter, quarter), quarter)

    def signal(sem, **device):
        pl.semaphore_signal(sem, inc=1, device_id=device, device_id_type=MESH)

    def remote(source, target, send, recv, **device):
        return pltpu.make_async_remote_copy(
            src_ref=source, dst_ref=target, send_sem=send, recv_sem=recv,
            device_id=device, device_id_type=MESH,
        )

    def span(piece):
        start, count = pieces[piece]
        return slice(start, start + count)

    def raw(piece, rows_device, lanes_side):
        return remote(
            ensemble.at[span(piece), :, lanes_of(lanes_side)],
            arrived.at[span(piece), rows_of(rows_device), :],
            raw_send.at[piece], raw_recv.at[piece], mem=far_hub,
        )

    def forward(piece, rows_device):
        return remote(
            relay.at[span(piece)], arrived.at[span(piece), rows_of(rows_device), :],
            forward_send.at[piece], forward_recv.at[piece], mem=far_hub,
        )

    def to_hub(piece):
        return remote(
            ensemble.at[span(piece), :, lanes_of(side)],
            arrived.at[span(piece), rows_of(own_end), :],
            end_send.at[piece], end_recv.at[piece], mem=own_hub,
        )

    def to_relay(piece):
        return remote(
            ensemble.at[span(piece), :, lanes_of(1 - side)], relay.at[span(piece)],
            relay_send.at[piece], relay_recv.at[piece], mem=own_hub,
        )

    def own_raw(piece):
        return pltpu.make_async_copy(
            ensemble.at[span(piece), :, lanes_of(side)],
            arrived.at[span(piece), rows_of(me), :],
            own_in.at[piece],
        )

    def outward(block, piece, send, recv, peer, columns):
        return remote(
            results.at[span(piece), block * local : (block + 1) * local, :],
            analysis.at[span(piece), :, lanes_of(columns)],
            send.at[piece], recv, mem=peer,
        )

    def to_beside(piece):
        return outward(0, piece, beside_send, out_recv.at[piece, side], own_end, side)

    def to_near(piece):
        return outward(1, piece, near_send, near_recv.at[piece], far_hub, side)

    def to_far(piece):
        return outward(2, piece, far_send, out_recv.at[piece, side], far_end, side)

    def from_side(piece, source):
        return outward(0, piece, beside_send, out_recv.at[piece, source], own_hub, source)

    loads = [
        pltpu.make_async_copy(source, target, small_sem.at[index])
        for index, (source, target) in enumerate(
            zip((transform_in, operator_in, weight_in), (transform, obs_operator, obs_weight))
        )
    ]
    barrier = pltpu.get_barrier_semaphore()

    @pl.when(is_hub)
    def _():
        signal(barrier, mem=far_hub)
        signal(barrier, mem=own_end)
        signal(barrier, mem=far_end)
        pl.semaphore_wait(barrier, 1)
        for piece in range(LEAD):
            raw(piece, me, 1 - side).start()
        for piece in order:
            own_raw(piece).start()

    @pl.when(is_end)
    def _():
        for peer in space_peers:
            signal(barrier, space=peer)
        pl.semaphore_wait(barrier, 2 + n_space - 1)
        to_relay(0).start()
        for piece in order:
            if piece + 1 < len(pieces):
                to_relay(piece + 1).start()
            to_hub(piece).start()
        for peer in space_peers:
            signal(met, space=peer)
        pl.semaphore_wait(met, n_space - 1)
        signal(ready, mem=own_hub)
        signal(ready, mem=far_hub)

    for load in loads:
        load.start()
    for load in loads:
        load.wait()
    eye = as_bf16(selector((members, members), lambda r, c: r == c))
    mixing_t = lax.dot_general(eye, transform[...], NT, preferred_element_type=jnp.float32)

    def device_of(block):
        outer = jnp.where(block == 1, own_end, far_end)
        inner = jnp.where(block == 0, own_hub, far_hub)
        return jnp.where(jnp.logical_or(block == 0, block == 2), inner, outer)

    def work():
        placed = as_bf16(selector(
            (members, members), lambda r, c: c == device_of(r // local) * local + lax.rem(r, local)
        ))
        ordered = lax.dot_general(placed, transform[...], NT, preferred_element_type=jnp.float32)
        keep = 1.0 - jnp.sum(ordered, axis=1, keepdims=True)
        ones = jnp.ones((ROWS, members), jnp.float32)
        mixer = jnp.concatenate([ordered, ones], axis=0).astype(jnp.bfloat16)

        obs_rows = n_obs * ROWS
        obs_pick = as_bf16(selector((obs_rows, n_obs), lambda r, c: r // ROWS == c))
        for piece, (start, count) in enumerate(pieces):
            depth = count * ROWS
            place = as_bf16(selector((variables, depth), lambda r, c: r == c // ROWS + start))
            part = dot(obs_operator[...], place).astype(jnp.bfloat16)
            mask = selector((obs_rows, depth), lambda r, c: lax.rem(r, ROWS) == lax.rem(c, ROWS))
            full = jnp.where(mask, dot(obs_pick, part), 0.0)
            observer[piece, :, 0:depth] = full.astype(jnp.bfloat16)

        def feed(piece):
            to_relay(piece).wait_recv()
            forward(piece, own_end).start()
            if piece + LEAD < len(pieces):
                raw(piece + LEAD, me, 1 - side).start()

        def take(piece):
            own_raw(piece).wait()
            to_hub(piece).wait_recv()
            raw(piece, far_hub, side).wait_recv()
            forward(piece, far_end).wait_recv()

        def mix(piece):
            start, count = pieces[piece]
            for variable in range(start, start + count):
                mixed = dot(mixer, arrived[variable])
                mean = mixed[members : members + 1, :] / members
                value = (mixed[:members, :] + keep * mean).astype(jnp.bfloat16)
                analysis[variable, :, lanes_of(side)] = value[0:local, :]
                results[variable] = value[local:, :]

        def observe(piece):
            start, count = pieces[piece]
            depth = count * ROWS
            for block in range(blocks):
                at = slice(block * ROWS, (block + 1) * ROWS)
                states = arrived[start : start + count, at, :].reshape(depth, half)
                term = dot(observer[piece, :, 0:depth], states).reshape(n_obs, ROWS, half)
                if piece == 0:
                    observed[:, at, :] = term
                else:
                    observed[:, at, :] += term

        def form_gram():
            weights = obs_weight[:, lanes_of(side)]
            total = jnp.zeros((members, members), jnp.float32)
            for quantity in range(n_obs):
                values = observed[quantity]
                departures = values - jnp.sum(values, axis=0, keepdims=True) / members
                total += lax.dot_general(
                    departures * weights[quantity : quantity + 1, :],
                    departures,
                    NT,
                    precision=HIGHEST,
                    preferred_element_type=jnp.float32,
                )
            gram[...] = jnp.full(gram.shape, jnp.sum(weights), jnp.float32)
            gram[:, 0:members] = total

        def to_part(peer, slot):
            return remote(
                gram.at[quarter_of(peer)], parts.at[slot],
                part_send.at[peer], part_recv.at[slot], space=peer,
            )

        def to_cross():
            return remote(summed, crossed, cross_send.at[0], cross_recv.at[0], mem=far_hub)

        def to_total(peer, source):
            return remote(
                totals.at[quarter_of(source)], totals.at[quarter_of(source)],
                total_send.at[peer], total_recv.at[source], space=peer,
            )

        steps = len(pieces)
        for piece in range(min(LEAD, steps)):
            feed(piece)
        fed = min(LEAD, steps)
        pl.semaphore_wait(ready, 2)
        behind = []
        for piece in order:
            take(piece)
            mix(piece)
            to_beside(piece).start()
            behind.append(piece)
            if fed < steps:
                feed(fed)
                fed += 1
            if fed == steps:
                for ahead in behind:
                    to_far(ahead).start()
                behind = []
            observe(piece)
        for piece in range(min(1, steps)):
            to_near(piece).start()
        form_gram()
        for peer in space_peers:
            to_part(peer, here).start()
        parts[here] = gram[quarter_of(here), :]
        for peer in space_peers:
            to_part(peer, peer).wait_recv()
        total = parts[0]
        for slot in range(1, n_space):
            total += parts[slot]
        summed[...] = total
        to_cross().start()
        for piece in range(min(1, steps), steps):
            to_near(piece).start()
        to_cross().wait_recv()
        totals[quarter_of(here), :] = total + crossed[...]
        for peer in space_peers:
            to_total(peer, here).start()
        for peer in space_peers:
            to_total(peer, peer).wait_recv()
        remote(totals, totals, last_send.at[0], last_recv.at[0], mem=own_end).start()
        for peer in space_peers:
            to_part(peer, here).wait_send()
            to_total(peer, here).wait_send()
        to_cross().wait_send()

    pl.when(is_hub)(work)

    @pl.when(is_end)
    def _():
        remote(totals, totals, last_send.at[0], last_recv.at[0], mem=own_hub).wait_recv()

    prior_gram = totals[:, 0:members] / totals[:, members : members + 1]
    prior[...] = prior_gram
    carried = jnp.dot(
        mixing_t, prior_gram, precision=HIGHEST, preferred_element_type=jnp.float32
    )
    posterior[...] = jnp.dot(
        carried,
        transform[...].astype(jnp.float32),
        precision=HIGHEST,
        preferred_element_type=jnp.float32,
    )

    @pl.when(is_hub)
    def _():
        remote(totals, totals, last_send.at[0], last_recv.at[0], mem=own_end).wait_send()
        for piece in order:
            raw(piece, me, 1 - side).wait_send()
            forward(piece, own_end).wait_send()
            to_beside(piece).wait_send()
            to_far(piece).wait_send()
            to_near(piece).wait_send()
        for piece in order:
            outward(1, piece, near_send, near_recv.at[piece], far_hub, 1 - side).wait_recv()

    @pl.when(is_end)
    def _():
        for piece in order:
            to_relay(piece).wait_send()
            to_hub(piece).wait_send()
        for piece in order:
            for source in range(2):
                from_side(piece, source).wait_recv()


def hub_call(n_mem, n_space, pieces, ensemble, transform, obs_operator, obs_weight):
    variables, local, cells = ensemble.shape
    members = transform.shape[0]
    n_obs = obs_operator.shape[0]
    half = cells // 2
    sizes = (n_mem, n_space, pieces, local, members, variables, n_obs, half)
    vmem = pl.BlockSpec(memory_space=pltpu.VMEM)
    any_space = pl.BlockSpec(memory_space=pl.ANY)
    dma = pltpu.SemaphoreType.DMA
    steps = len(pieces)
    quarter = members // n_space
    return pl.pallas_call(
        functools.partial(hub_kernel, sizes),
        out_shape=(
            pltpu.VMEM((variables, local, cells), jnp.bfloat16),
            pltpu.VMEM((members, members), jnp.float32),
            pltpu.VMEM((members, members), jnp.float32),
        ),
        in_specs=[any_space] * 4,
        out_specs=(vmem, vmem, vmem),
        scratch_shapes=[
            pltpu.VMEM(transform.shape, jnp.bfloat16),
            pltpu.VMEM(obs_operator.shape, jnp.bfloat16),
            pltpu.VMEM(obs_weight.shape, jnp.float32),
            dma((3,)),
            pltpu.VMEM((variables, members, half), jnp.bfloat16),
            pltpu.VMEM((variables, local, half), jnp.bfloat16),
            pltpu.VMEM((variables, members - local, half), jnp.bfloat16),
            pltpu.VMEM((steps, n_obs * ROWS, PIECE * ROWS), jnp.bfloat16),
            pltpu.VMEM((n_obs, members, half), jnp.float32),
            pltpu.VMEM((members, LANES), jnp.float32),
            pltpu.VMEM((n_space, quarter, LANES), jnp.float32),
            pltpu.VMEM((quarter, LANES), jnp.float32),
            pltpu.VMEM((quarter, LANES), jnp.float32),
            pltpu.VMEM((members, LANES), jnp.float32),
        ]
        + [dma((steps,))] * 12
        + [dma((steps, 2)), dma((steps,))]
        + [dma((n_space,)), dma((n_space,)), dma((1,)), dma((1,))]
        + [dma((n_space,)), dma((n_space,)), dma((1,)), dma((1,))]
        + [pltpu.SemaphoreType.REGULAR, pltpu.SemaphoreType.REGULAR],
        compiler_params=pltpu.CompilerParams(collective_id=0, has_side_effects=True),
        name="hub_exchange",
    )(ensemble, transform, obs_operator, obs_weight)


def store(*refs):
    count = len(refs) // 2
    sources, targets, sems = refs[:count], refs[count : 2 * count], refs[-1]
    pairs = []
    for source, target in zip(sources, targets):
        if len(source.shape) == 3:
            for start in range(0, source.shape[0], PIECE):
                part = slice(start, min(start + PIECE, source.shape[0]))
                pairs.append((source.at[part], target.at[part]))
        else:
            pairs.append((source, target))
    copies = [
        pltpu.make_async_copy(source, target, sems.at[index])
        for index, (source, target) in enumerate(pairs)
    ]
    for copy in copies:
        copy.start()
    for copy in copies:
        copy.wait()


def write_out(*arrays):
    return pl.pallas_call(
        store,
        out_shape=tuple(jax.ShapeDtypeStruct(a.shape, a.dtype) for a in arrays),
        in_specs=[pl.BlockSpec(memory_space=pl.ANY)] * len(arrays),
        out_specs=tuple([pl.BlockSpec(memory_space=pl.ANY)] * len(arrays)),
        scratch_shapes=[pltpu.SemaphoreType.DMA((len(arrays) + pl.cdiv(arrays[0].shape[0], PIECE),))],
        compiler_params=pltpu.CompilerParams(vmem_limit_bytes=8 << 20),
        name="store_outputs",
    )(*arrays)


def per_device(n_mem, n_space, ensemble, transform, obs_operator, obs_weight):
    local, variables, cells = ensemble.shape
    members = transform.shape[0]
    n_obs = obs_operator.shape[0]
    active = min(n_mem, cells // LANES)
    chunk = cells // active
    pieces = tuple(
        (start, min(PIECE, variables - start)) for start in range(0, variables, PIECE)
    )
    if (
        n_mem == 4
        and local == ROWS
        and members < LANES
        and members % (8 * n_space) == 0
        and cells % (2 * LANES) == 0
    ):
        by_variable, prior, posterior = write_out(*hub_call(
            n_mem, n_space, pieces, jnp.transpose(ensemble, (1, 0, 2)), transform, obs_operator, obs_weight
        ))
        return jnp.transpose(by_variable, (1, 0, 2)), prior, posterior
    sizes = (n_mem, n_space, active, pieces, local, members, variables, n_obs, chunk)
    vmem = pl.BlockSpec(memory_space=pltpu.VMEM)
    any_space = pl.BlockSpec(memory_space=pl.ANY)
    gram_shape = (members + 8, LANES)
    slabs = (1, 1, ROWS, LANES) if local % ROWS == 0 else (n_mem, variables, local, chunk)
    dma = pltpu.SemaphoreType.DMA
    by_variable, prior, posterior = pl.pallas_call(
        functools.partial(line_kernel, sizes),
        out_shape=(
            pltpu.VMEM((variables, local, cells), jnp.bfloat16),
            pltpu.VMEM((members, members), jnp.float32),
            pltpu.VMEM((members, members), jnp.float32),
        ),
        in_specs=[any_space] * 4,
        out_specs=(vmem, vmem, vmem),
        scratch_shapes=[
            pltpu.VMEM(transform.shape, jnp.bfloat16),
            pltpu.VMEM(obs_operator.shape, jnp.bfloat16),
            pltpu.VMEM(obs_weight.shape, jnp.float32),
            dma((3,)),
            pltpu.VMEM((variables, members, chunk), jnp.bfloat16),
            pltpu.VMEM((variables, members, chunk), jnp.bfloat16),
            pltpu.VMEM((len(pieces), n_obs * ROWS, PIECE * ROWS), jnp.bfloat16),
            pltpu.VMEM((n_obs, members, chunk), jnp.float32),
            pltpu.VMEM(gram_shape, jnp.float32),
            pltpu.VMEM((n_space,) + gram_shape, jnp.float32),
            pltpu.VMEM((n_mem,) + gram_shape, jnp.float32),
            pltpu.VMEM(slabs, jnp.bfloat16),
            pltpu.VMEM(slabs, jnp.bfloat16),
            dma((len(pieces), n_mem)),
            dma((len(pieces), n_mem)),
            dma((len(pieces), n_mem)),
            dma((len(pieces), n_mem)),
            dma((len(pieces),)),
            dma((len(pieces),)),
            dma((n_space,)),
            dma((n_space,)),
            dma((n_mem,)),
            dma((n_mem,)),
        ],
        compiler_params=pltpu.CompilerParams(collective_id=0, has_side_effects=True),
        name="ensemble_exchange",
    )(jnp.transpose(ensemble, (1, 0, 2)), transform, obs_operator, obs_weight)
    by_variable, prior, posterior = write_out(by_variable, prior, posterior)
    return jnp.transpose(by_variable, (1, 0, 2)), prior, posterior


def solution(mesh):
    return jax.shard_map(
        functools.partial(per_device, mesh.shape["mem"], mesh.shape["space"]),
        mesh=mesh,
        in_specs=(
            P("mem", None, ("parts", "space")),
            P("parts", None),
            P(),
            P(None, ("parts", "space")),
        ),
        out_specs=(P("mem", None, ("parts", "space")), P("parts", None), P("parts", None)),
        check_vma=False,
    )
```

```python
import functools

import jax
import jax.numpy as jnp
from jax import lax
from jax.experimental import pallas as pl
from jax.experimental.pallas import tpu as pltpu
from jax.sharding import PartitionSpec as P

HIGHEST = lax.Precision.HIGHEST
MESH = pl.DeviceIdType.MESH
LANES = 128
PIECE = 14
ROWS = 16
LEAD = 2
SENT, OUT, FINAL, PART, TOTAL, CROSS, LAST, SMALL = range(8)
NT = (((1,), (1,)), ((), ()))


def dot(a, b):
    return jnp.dot(a, b, preferred_element_type=jnp.float32)


def selector(shape, match):
    rows = lax.broadcasted_iota(jnp.int32, shape, 0)
    cols = lax.broadcasted_iota(jnp.int32, shape, 1)
    return match(rows, cols)


def as_bf16(mask):
    return jnp.where(mask, 1.0, 0.0).astype(jnp.bfloat16)


def peers_of(me, size):
    if size % 2:
        return [lax.rem(me + step, size) for step in range(1, size)], []
    half = size // 2
    side, place = me // half, lax.rem(me, half)
    across = [(1 - side) * half + lax.rem(place + step, half) for step in range(half)]
    return across, [side * half + lax.rem(place + step, half) for step in range(1, half)]


def when(needed, condition, body):
    if needed:
        pl.when(condition)(body)
    else:
        body()


def line_kernel(
    sizes, ensemble, *refs,
):
    smalls, refs = refs[:3], refs[3:]
    analysis, prior, posterior, transform, obs_operator, obs_weight, small_sem = refs[:7]
    (
    arrived, results, observer, observed, gram, by_space, by_mem, in_slabs, out_slabs,
    in_send, in_recv, out_send, out_recv, own_in, own_out,
    space_send, space_recv, mem_send, mem_recv,
    ) = refs[7:]
    n_mem, n_space, active, pieces, local, members, variables, n_obs, chunk = sizes
    blocks = members // ROWS
    aligned = local % ROWS == 0
    partial_owners = active < n_mem
    me = lax.axis_index("mem")
    here = lax.axis_index("space")
    across, beside = peers_of(me, n_mem)
    mem_peers = across + beside
    space_peers = sum(peers_of(here, n_space), [])
    central = jnp.logical_or(me * 2 == n_mem, (me + 1) * 2 == n_mem)

    def lanes_of(owner):
        return pl.ds(pl.multiple_of(owner * chunk, chunk), chunk)

    def rows_of(device):
        return pl.ds(pl.multiple_of(device * local, local), local)

    barrier = pltpu.get_barrier_semaphore()
    for peer in mem_peers:
        pl.semaphore_signal(barrier, inc=1, device_id={"mem": peer}, device_id_type=MESH)
    for peer in space_peers:
        pl.semaphore_signal(barrier, inc=1, device_id={"space": peer}, device_id_type=MESH)
    pl.semaphore_wait(barrier, n_mem - 1 + n_space - 1)

    def spot(whole, slabs, piece, device):
        start, count = pieces[piece]
        if aligned:
            return whole.at[start : start + count, rows_of(device), :]
        return slabs.at[device, start : start + count]

    def outside(array, piece, owner):
        start, count = pieces[piece]
        return array.at[start : start + count, :, lanes_of(owner)]

    def inward(piece, peer, source):
        return pltpu.make_async_remote_copy(
            src_ref=outside(ensemble, piece, peer),
            dst_ref=spot(arrived, in_slabs, piece, source),
            send_sem=in_send.at[piece, peer],
            recv_sem=in_recv.at[piece, source],
            device_id={"mem": peer},
            device_id_type=MESH,
        )

    def inward_own(piece):
        return pltpu.make_async_copy(
            outside(ensemble, piece, me), spot(arrived, in_slabs, piece, me), own_in.at[piece]
        )

    def outward(piece, peer, owner):
        return pltpu.make_async_remote_copy(
            src_ref=spot(results, out_slabs, piece, peer),
            dst_ref=outside(analysis, piece, owner),
            send_sem=out_send.at[piece, peer],
            recv_sem=out_recv.at[piece, owner],
            device_id={"mem": peer},
            device_id_type=MESH,
        )

    def outward_own(piece):
        return pltpu.make_async_copy(
            spot(results, out_slabs, piece, me), outside(analysis, piece, me), own_out.at[piece]
        )

    owns = me < active
    for group in (beside, across):
        for piece in range(len(pieces)):
            for peer in group:
                when(partial_owners, peer < active, lambda: inward(piece, peer, me).start())
    for piece in range(len(pieces)):
        when(partial_owners, owns, lambda: inward_own(piece).start())
    loads = [
        pltpu.make_async_copy(source, target, small_sem.at[index])
        for index, (source, target) in enumerate(
            zip(smalls, (transform, obs_operator, obs_weight))
        )
    ]
    for load in loads:
        load.start()
    for load in loads:
        load.wait()

    eye = as_bf16(selector((members, members), lambda r, c: r == c))
    mixing_t = lax.dot_general(eye, transform[...], NT, preferred_element_type=jnp.float32)
    keep = 1.0 - jnp.sum(mixing_t, axis=1, keepdims=True)
    ones = jnp.ones((ROWS, members), jnp.float32)
    mixer = jnp.concatenate([mixing_t, ones], axis=0).astype(jnp.bfloat16)

    obs_rows = n_obs * ROWS
    obs_pick = as_bf16(selector((obs_rows, n_obs), lambda r, c: r // ROWS == c))
    for piece, (start, count) in enumerate(pieces):
        depth = count * ROWS
        place = as_bf16(selector((variables, depth), lambda r, c: r == c // ROWS + start))
        part = dot(obs_operator[...], place).astype(jnp.bfloat16)
        mask = selector((obs_rows, depth), lambda r, c: lax.rem(r, ROWS) == lax.rem(c, ROWS))
        full = jnp.where(mask, dot(obs_pick, part), 0.0)
        observer[piece, :, 0:depth] = full.astype(jnp.bfloat16)

    def mix(piece):
        start, count = pieces[piece]
        for variable in range(start, start + count):
            if not aligned:
                for device in range(n_mem):
                    rows = slice(device * local, (device + 1) * local)
                    arrived[variable, rows, :] = in_slabs[device, variable]
            mixed = dot(mixer, arrived[variable])
            mean = mixed[members : members + 1, :] / members
            value = (mixed[:members, :] + keep * mean).astype(jnp.bfloat16)
            if aligned:
                results[variable] = value
            else:
                for device in range(n_mem):
                    rows = slice(device * local, (device + 1) * local)
                    out_slabs[device, variable] = value[rows, :]

    def observe(piece):
        start, count = pieces[piece]
        depth = count * ROWS
        for block in range(blocks):
            at = slice(block * ROWS, (block + 1) * ROWS)
            states = arrived[start : start + count, at, :].reshape(depth, chunk)
            term = dot(observer[piece, :, 0:depth], states).reshape(n_obs, ROWS, chunk)
            if piece == 0:
                observed[:, at, :] = term
            else:
                observed[:, at, :] += term

    def form_gram():
        weights = obs_weight[:, lanes_of(me)]
        total = jnp.zeros((members, members), jnp.float32)
        for quantity in range(n_obs):
            values = observed[quantity]
            departures = values - jnp.sum(values, axis=0, keepdims=True) / members
            total += lax.dot_general(
                departures * weights[quantity : quantity + 1, :],
                departures,
                NT,
                precision=HIGHEST,
                preferred_element_type=jnp.float32,
            )
        gram[0:members, 0:members] = total
        gram[members : members + 8, :] = jnp.full((8, LANES), jnp.sum(weights), jnp.float32)

    gram[...] = jnp.zeros_like(gram)

    last = len(pieces) - 1

    def send_back(piece, group):
        for peer in group:
            outward(piece, peer, me).start()

    def work():
        for piece in range(last + 1):
            for peer in mem_peers:
                inward(piece, me, peer).wait_recv()
            inward_own(piece).wait()
            mix(piece)
            send_back(piece, beside)
            if piece < last:
                pl.when(central)(lambda: send_back(piece, across))
            outward_own(piece).start()
            observe(piece)
        form_gram()

    def finish_sends():
        for piece in range(last):
            pl.when(jnp.logical_not(central))(lambda: send_back(piece, across))
        send_back(last, across)

    when(partial_owners, owns, work)

    def exchange(source, slots, index, peers, axis, send, recv, between):
        slots[index] = source
        copies = [
            pltpu.make_async_remote_copy(
                src_ref=slots.at[index],
                dst_ref=slots.at[index],
                send_sem=send.at[peer],
                recv_sem=recv.at[index],
                device_id={axis: peer},
                device_id_type=MESH,
            )
            for peer in peers
        ]
        for copy in copies:
            copy.start()
        between()
        for peer in peers:
            pltpu.make_async_remote_copy(
                src_ref=slots.at[peer],
                dst_ref=slots.at[peer],
                send_sem=send.at[peer],
                recv_sem=recv.at[peer],
                device_id={axis: peer},
                device_id_type=MESH,
            ).wait_recv()
        total = slots[0]
        for slot in range(1, slots.shape[0]):
            total += slots[slot]
        for copy in copies:
            copy.wait_send()
        return total

    total = exchange(
        gram[...], by_space, here, space_peers, "space", space_send, space_recv, lambda: None
    )
    total = exchange(
        total, by_mem, me, mem_peers, "mem", mem_send, mem_recv,
        lambda: when(partial_owners, owns, finish_sends),
    )
    prior_gram = total[0:members, 0:members] / total[members : members + 1, 0:members]
    prior[...] = prior_gram
    carried = jnp.dot(
        mixing_t, prior_gram, precision=HIGHEST, preferred_element_type=jnp.float32
    )
    posterior[...] = jnp.dot(
        carried,
        transform[...].astype(jnp.float32),
        precision=HIGHEST,
        preferred_element_type=jnp.float32,
    )

    for piece in range(len(pieces)):
        for peer in mem_peers:
            when(partial_owners, peer < active, lambda: inward(piece, peer, me).wait_send())
            when(partial_owners, owns, lambda: outward(piece, peer, me).wait_send())
            when(partial_owners, peer < active, lambda: outward(piece, me, peer).wait_recv())
        when(partial_owners, owns, lambda: outward_own(piece).wait())


def hub_kernel(
    sizes, ensemble, transform_in, operator_in, weight_in, analysis, prior, posterior,
    transform, obs_operator, obs_weight, arrived, relay, results, observer, observed,
    gram, parts, summed, crossed, totals, sem, arrive, passing, met, ready,
):
    n_mem, n_space, pieces, local, members, variables, n_obs, half = sizes
    blocks = members // ROWS
    quarter = members // n_space
    me = lax.axis_index("mem")
    here = lax.axis_index("space")
    side = me // (n_mem // 2)
    is_hub = jnp.logical_or(me * 2 == n_mem, (me + 1) * 2 == n_mem)
    is_end = jnp.logical_not(is_hub)
    last_mem = n_mem - 1
    own_hub, far_hub = 1 + side, 2 - side
    own_end, far_end = last_mem * side, last_mem - last_mem * side
    space_peers = [lax.rem(here + step, n_space) for step in range(1, n_space)]
    order = range(len(pieces))

    def lanes_of(which):
        return pl.ds(pl.multiple_of(which * half, half), half)

    def rows_of(device):
        return pl.ds(pl.multiple_of(device * local, local), local)

    def quarter_of(device):
        return pl.ds(pl.multiple_of(device * quarter, quarter), quarter)

    def signal(sem, **device):
        pl.semaphore_signal(sem, inc=1, device_id=device, device_id_type=MESH)

    def remote(source, target, send, recv, **device):
        return pltpu.make_async_remote_copy(
            src_ref=source, dst_ref=target, send_sem=send, recv_sem=recv,
            device_id=device, device_id_type=MESH,
        )

    def span(piece):
        start, count = pieces[piece]
        return slice(start, start + count)

    def raw(piece, source, lanes_side):
        return remote(
            ensemble.at[span(piece), :, lanes_of(lanes_side)],
            arrived.at[span(piece), rows_of(source), :],
            sem.at[SENT], arrive.at[piece], mem=far_hub,
        )

    def forward(piece, source):
        return remote(
            relay.at[span(piece)], arrived.at[span(piece), rows_of(source), :],
            sem.at[SENT], arrive.at[piece], mem=far_hub,
        )

    def to_hub(piece):
        return remote(
            ensemble.at[span(piece), :, lanes_of(side)],
            arrived.at[span(piece), rows_of(own_end), :],
            sem.at[SENT], arrive.at[piece], mem=own_hub,
        )

    def to_relay(piece):
        return remote(
            ensemble.at[span(piece), :, lanes_of(1 - side)], relay.at[span(piece)],
            sem.at[SENT], passing.at[piece], mem=own_hub,
        )

    def own_raw(piece):
        return pltpu.make_async_copy(
            ensemble.at[span(piece), :, lanes_of(side)],
            arrived.at[span(piece), rows_of(me), :],
            arrive.at[piece],
        )

    def outward(block, piece, peer):
        return remote(
            results.at[span(piece), block * local : (block + 1) * local, :],
            analysis.at[span(piece), :, lanes_of(side)],
            sem.at[OUT], sem.at[FINAL], mem=peer,
        )

    def to_end():
        return remote(totals, totals, sem.at[LAST], sem.at[CROSS], mem=own_end)

    def landed(ref, semaphore):
        remote(ref, ref, semaphore, semaphore, mem=far_hub).wait_recv()

    def left(ref, semaphore):
        remote(ref, ref, semaphore, semaphore, mem=far_hub).wait_send()

    loads = [
        pltpu.make_async_copy(source, target, sem.at[SMALL + index])
        for index, (source, target) in enumerate(
            zip((transform_in, operator_in, weight_in), (transform, obs_operator, obs_weight))
        )
    ]
    barrier = pltpu.get_barrier_semaphore()

    @pl.when(is_hub)
    def _():
        signal(barrier, mem=far_hub)
        pl.semaphore_wait(barrier, 1)
        for piece in range(LEAD):
            raw(piece, me, 1 - side).start()
        signal(barrier, mem=own_end)
        signal(barrier, mem=far_end)
        for piece in order:
            own_raw(piece).start()

    @pl.when(is_end)
    def _():
        for peer in space_peers:
            signal(barrier, space=peer)
        pl.semaphore_wait(barrier, 2 + n_space - 1)
        to_relay(0).start()
        for piece in order:
            if piece + 1 < len(pieces):
                to_relay(piece + 1).start()
            to_hub(piece).start()
        for peer in space_peers:
            signal(met, space=peer)
        pl.semaphore_wait(met, n_space - 1)
        signal(ready, mem=own_hub)
        signal(ready, mem=far_hub)

    for load in loads:
        load.start()
    for load in loads:
        load.wait()
    eye = as_bf16(selector((members, members), lambda r, c: r == c))
    mixing_t = lax.dot_general(eye, transform[...], NT, preferred_element_type=jnp.float32)

    def device_of(block):
        outer = jnp.where(block == 1, own_end, far_end)
        inner = jnp.where(block == 0, own_hub, far_hub)
        return jnp.where(jnp.logical_or(block == 0, block == 2), inner, outer)

    def work():
        placed = as_bf16(selector(
            (members, members), lambda r, c: c == device_of(r // local) * local + lax.rem(r, local)
        ))
        ordered = lax.dot_general(placed, transform[...], NT, preferred_element_type=jnp.float32)
        keep = 1.0 - jnp.sum(ordered, axis=1, keepdims=True)
        ones = jnp.ones((ROWS, members), jnp.float32)
        mixer = jnp.concatenate([ordered, ones], axis=0).astype(jnp.bfloat16)

        obs_rows = n_obs * ROWS
        obs_pick = as_bf16(selector((obs_rows, n_obs), lambda r, c: r // ROWS == c))
        for piece, (start, count) in enumerate(pieces):
            depth = count * ROWS
            place = as_bf16(selector((variables, depth), lambda r, c: r == c // ROWS + start))
            part = dot(obs_operator[...], place).astype(jnp.bfloat16)
            mask = selector((obs_rows, depth), lambda r, c: lax.rem(r, ROWS) == lax.rem(c, ROWS))
            full = jnp.where(mask, dot(obs_pick, part), 0.0)
            observer[piece, :, 0:depth] = full.astype(jnp.bfloat16)

        def feed(piece):
            landed(relay.at[span(piece)], passing.at[piece])
            forward(piece, own_end).start()
            if piece + LEAD < len(pieces):
                raw(piece + LEAD, me, 1 - side).start()

        def take(piece):
            landed(arrived.at[span(piece)], arrive.at[piece])

        def mix(piece):
            start, count = pieces[piece]

            def several(step, carry):
                for offset in range(2):
                    variable = start + step * 2 + offset
                    mixed = dot(mixer, arrived[variable])
                    mean = mixed[members : members + 1, :] / members
                    value = (mixed[:members, :] + keep * mean).astype(jnp.bfloat16)
                    analysis[variable, :, lanes_of(side)] = value[0:local, :]
                    results[variable] = value[local:, :]
                return carry

            lax.fori_loop(0, count // 2, several, 0)

        def observe(piece):
            start, count = pieces[piece]
            depth = count * ROWS
            def one(block, carry):
                at = pl.ds(pl.multiple_of(block * ROWS, ROWS), ROWS)
                states = arrived[start : start + count, at, :].reshape(depth, half)
                term = dot(observer[piece, :, 0:depth], states).reshape(n_obs, ROWS, half)
                if piece == 0:
                    observed[:, at, :] = term
                else:
                    observed[:, at, :] += term
                return carry

            lax.fori_loop(0, blocks, one, 0)

        def form_gram():
            weights = obs_weight[:, lanes_of(side)]
            def one(quantity, total):
                values = observed[quantity]
                departures = values - jnp.sum(values, axis=0, keepdims=True) / members
                weight = obs_weight[pl.ds(quantity, 1), lanes_of(side)]
                return total + lax.dot_general(
                    departures * weight,
                    departures,
                    NT,
                    precision=HIGHEST,
                    preferred_element_type=jnp.float32,
                )

            total = lax.fori_loop(0, n_obs, one, jnp.zeros((members, members), jnp.float32))
            gram[...] = jnp.full(gram.shape, jnp.sum(weights), jnp.float32)
            gram[:, 0:members] = total

        def to_part(peer):
            return remote(
                gram.at[quarter_of(peer)], parts.at[here],
                sem.at[SMALL], sem.at[PART], space=peer,
            )

        def to_total(peer):
            return remote(
                totals.at[quarter_of(here)], totals.at[quarter_of(here)],
                sem.at[SMALL + 1], sem.at[TOTAL], space=peer,
            )

        to_cross = remote(summed, crossed, sem.at[SMALL + 2], sem.at[CROSS], mem=far_hub)
        others = (n_space - 1) * quarter
        steps = len(pieces)
        for piece in range(min(LEAD, steps)):
            feed(piece)
        fed = min(LEAD, steps)
        pl.semaphore_wait(ready, 2)
        behind = []
        for piece in order:
            take(piece)
            mix(piece)
            outward(0, piece, own_end).start()
            behind.append(piece)
            if fed < steps:
                feed(fed)
                fed += 1
            if fed == steps:
                for ahead in behind:
                    outward(2, ahead, far_end).start()
                behind = []
            observe(piece)
        outward(1, 0, far_hub).start()
        form_gram()
        for peer in space_peers:
            to_part(peer).start()
        parts[here] = gram[quarter_of(here), :]
        landed(parts.at[0 : n_space - 1], sem.at[PART])
        total = parts[0]
        for slot in range(1, n_space):
            total += parts[slot]
        summed[...] = total
        to_cross.start()
        for piece in order[1:]:
            outward(1, piece, far_hub).start()
        to_cross.wait_recv()
        totals[quarter_of(here), :] = total + crossed[...]
        for peer in space_peers:
            to_total(peer).start()
        landed(totals.at[0:others], sem.at[TOTAL])
        to_end().start()
        left(gram.at[0:others], sem.at[SMALL])
        left(totals.at[0:others], sem.at[SMALL + 1])
        to_cross.wait_send()

    pl.when(is_hub)(work)

    @pl.when(is_end)
    def _():
        to_end().wait_recv()

    prior_gram = totals[:, 0:members] / totals[:, members : members + 1]
    prior[...] = prior_gram
    carried = jnp.dot(
        mixing_t, prior_gram, precision=HIGHEST, preferred_element_type=jnp.float32
    )
    posterior[...] = jnp.dot(
        carried,
        transform[...].astype(jnp.float32),
        precision=HIGHEST,
        preferred_element_type=jnp.float32,
    )

    left(ensemble, sem.at[SENT])

    @pl.when(is_hub)
    def _():
        to_end().wait_send()
        left(results, sem.at[OUT])
        landed(analysis.at[:, :, lanes_of(1 - side)], sem.at[FINAL])

    @pl.when(is_end)
    def _():
        landed(analysis, sem.at[FINAL])


def hub_call(n_mem, n_space, pieces, ensemble, transform, obs_operator, obs_weight):
    variables, local, cells = ensemble.shape
    members = transform.shape[0]
    n_obs = obs_operator.shape[0]
    half = cells // 2
    sizes = (n_mem, n_space, pieces, local, members, variables, n_obs, half)
    vmem = pl.BlockSpec(memory_space=pltpu.VMEM)
    any_space = pl.BlockSpec(memory_space=pl.ANY)
    dma = pltpu.SemaphoreType.DMA
    steps = len(pieces)
    quarter = members // n_space
    return pl.pallas_call(
        functools.partial(hub_kernel, sizes),
        out_shape=(
            pltpu.VMEM((variables, local, cells), jnp.bfloat16),
            pltpu.VMEM((members, members), jnp.float32),
            pltpu.VMEM((members, members), jnp.float32),
        ),
        in_specs=[any_space] * 4,
        out_specs=(vmem, vmem, vmem),
        scratch_shapes=[
            pltpu.VMEM(transform.shape, jnp.bfloat16),
            pltpu.VMEM(obs_operator.shape, jnp.bfloat16),
            pltpu.VMEM(obs_weight.shape, jnp.float32),
            pltpu.VMEM((variables, members, half), jnp.bfloat16),
            pltpu.VMEM((variables, local, half), jnp.bfloat16),
            pltpu.VMEM((variables, members - local, half), jnp.bfloat16),
            pltpu.VMEM((steps, n_obs * ROWS, PIECE * ROWS), jnp.bfloat16),
            pltpu.VMEM((n_obs, members, half), jnp.float32),
            pltpu.VMEM((members, LANES), jnp.float32),
            pltpu.VMEM((n_space, quarter, LANES), jnp.float32),
            pltpu.VMEM((quarter, LANES), jnp.float32),
            pltpu.VMEM((quarter, LANES), jnp.float32),
            pltpu.VMEM((members, LANES), jnp.float32),
            dma((SMALL + 3,)),
            dma((steps,)),
            dma((steps,)),
            pltpu.SemaphoreType.REGULAR,
            pltpu.SemaphoreType.REGULAR,
        ],
        compiler_params=pltpu.CompilerParams(collective_id=0, has_side_effects=True),
        name="hub_exchange",
    )(ensemble, transform, obs_operator, obs_weight)


def store(*refs):
    count = len(refs) // 2
    sources, targets, sems = refs[:count], refs[count : 2 * count], refs[-1]
    copies = [
        pltpu.make_async_copy(source, target, sems.at[index])
        for index, (source, target) in enumerate(zip(sources, targets))
    ]
    for copy in copies:
        copy.start()
    for copy in copies:
        copy.wait()


def write_out(*arrays):
    return pl.pallas_call(
        store,
        out_shape=tuple(jax.ShapeDtypeStruct(a.shape, a.dtype) for a in arrays),
        in_specs=[pl.BlockSpec(memory_space=pl.ANY)] * len(arrays),
        out_specs=tuple([pl.BlockSpec(memory_space=pl.ANY)] * len(arrays)),
        scratch_shapes=[pltpu.SemaphoreType.DMA((len(arrays),))],
        compiler_params=pltpu.CompilerParams(vmem_limit_bytes=8 << 20),
        name="store_outputs",
    )(*arrays)


def per_device(n_mem, n_space, ensemble, transform, obs_operator, obs_weight):
    local, variables, cells = ensemble.shape
    members = transform.shape[0]
    n_obs = obs_operator.shape[0]
    active = min(n_mem, cells // LANES)
    chunk = cells // active
    pieces = tuple(
        (start, min(PIECE, variables - start)) for start in range(0, variables, PIECE)
    )
    if (
        n_mem == 4
        and local == ROWS
        and members < LANES
        and members % (8 * n_space) == 0
        and cells % (2 * LANES) == 0
    ):
        by_variable, prior, posterior = write_out(*hub_call(
            n_mem, n_space, pieces, jnp.transpose(ensemble, (1, 0, 2)), transform, obs_operator, obs_weight
        ))
        return jnp.transpose(by_variable, (1, 0, 2)), prior, posterior
    sizes = (n_mem, n_space, active, pieces, local, members, variables, n_obs, chunk)
    vmem = pl.BlockSpec(memory_space=pltpu.VMEM)
    any_space = pl.BlockSpec(memory_space=pl.ANY)
    gram_shape = (members + 8, LANES)
    slabs = (1, 1, ROWS, LANES) if local % ROWS == 0 else (n_mem, variables, local, chunk)
    dma = pltpu.SemaphoreType.DMA
    by_variable, prior, posterior = pl.pallas_call(
        functools.partial(line_kernel, sizes),
        out_shape=(
            pltpu.VMEM((variables, local, cells), jnp.bfloat16),
            pltpu.VMEM((members, members), jnp.float32),
            pltpu.VMEM((members, members), jnp.float32),
        ),
        in_specs=[any_space] * 4,
        out_specs=(vmem, vmem, vmem),
        scratch_shapes=[
            pltpu.VMEM(transform.shape, jnp.bfloat16),
            pltpu.VMEM(obs_operator.shape, jnp.bfloat16),
            pltpu.VMEM(obs_weight.shape, jnp.float32),
            dma((3,)),
            pltpu.VMEM((variables, members, chunk), jnp.bfloat16),
            pltpu.VMEM((variables, members, chunk), jnp.bfloat16),
            pltpu.VMEM((len(pieces), n_obs * ROWS, PIECE * ROWS), jnp.bfloat16),
            pltpu.VMEM((n_obs, members, chunk), jnp.float32),
            pltpu.VMEM(gram_shape, jnp.float32),
            pltpu.VMEM((n_space,) + gram_shape, jnp.float32),
            pltpu.VMEM((n_mem,) + gram_shape, jnp.float32),
            pltpu.VMEM(slabs, jnp.bfloat16),
            pltpu.VMEM(slabs, jnp.bfloat16),
            dma((len(pieces), n_mem)),
            dma((len(pieces), n_mem)),
            dma((len(pieces), n_mem)),
            dma((len(pieces), n_mem)),
            dma((len(pieces),)),
            dma((len(pieces),)),
            dma((n_space,)),
            dma((n_space,)),
            dma((n_mem,)),
            dma((n_mem,)),
        ],
        compiler_params=pltpu.CompilerParams(collective_id=0, has_side_effects=True),
        name="ensemble_exchange",
    )(jnp.transpose(ensemble, (1, 0, 2)), transform, obs_operator, obs_weight)
    by_variable, prior, posterior = write_out(by_variable, prior, posterior)
    return jnp.transpose(by_variable, (1, 0, 2)), prior, posterior


def solution(mesh):
    return jax.shard_map(
        functools.partial(per_device, mesh.shape["mem"], mesh.shape["space"]),
        mesh=mesh,
        in_specs=(
            P("mem", None, ("parts", "space")),
            P("parts", None),
            P(),
            P(None, ("parts", "space")),
        ),
        out_specs=(P("mem", None, ("parts", "space")), P("parts", None), P("parts", None)),
        check_vma=False,
    )
```

```python
import functools

import jax
import jax.numpy as jnp
from jax import lax
from jax.experimental import pallas as pl
from jax.experimental.pallas import tpu as pltpu
from jax.sharding import PartitionSpec as P

HIGHEST = lax.Precision.HIGHEST
MESH = pl.DeviceIdType.MESH
LANES = 128
PIECE = 14
ROWS = 16
LEAD = 2
SENT, OUT, LAST, SMALL, FINAL, PART, TOTAL, CROSS = range(8)
NT = (((1,), (1,)), ((), ()))


def dot(a, b):
    return jnp.dot(a, b, preferred_element_type=jnp.float32)


def selector(shape, match):
    rows = lax.broadcasted_iota(jnp.int32, shape, 0)
    cols = lax.broadcasted_iota(jnp.int32, shape, 1)
    return match(rows, cols)


def as_bf16(mask):
    return jnp.where(mask, 1.0, 0.0).astype(jnp.bfloat16)


def peers_of(me, size):
    if size % 2:
        return [lax.rem(me + step, size) for step in range(1, size)], []
    half = size // 2
    side, place = me // half, lax.rem(me, half)
    across = [(1 - side) * half + lax.rem(place + step, half) for step in range(half)]
    return across, [side * half + lax.rem(place + step, half) for step in range(1, half)]


def when(needed, condition, body):
    if needed:
        pl.when(condition)(body)
    else:
        body()


def line_kernel(
    sizes, ensemble, *refs,
):
    smalls, refs = refs[:3], refs[3:]
    analysis, prior, posterior, transform, obs_operator, obs_weight, small_sem = refs[:7]
    (
    arrived, results, observer, observed, gram, by_space, by_mem, in_slabs, out_slabs,
    in_send, in_recv, out_send, out_recv, own_in, own_out,
    space_send, space_recv, mem_send, mem_recv,
    ) = refs[7:]
    n_mem, n_space, active, pieces, local, members, variables, n_obs, chunk = sizes
    blocks = members // ROWS
    aligned = local % ROWS == 0
    partial_owners = active < n_mem
    me = lax.axis_index("mem")
    here = lax.axis_index("space")
    across, beside = peers_of(me, n_mem)
    mem_peers = across + beside
    space_peers = sum(peers_of(here, n_space), [])
    central = jnp.logical_or(me * 2 == n_mem, (me + 1) * 2 == n_mem)

    def lanes_of(owner):
        return pl.ds(pl.multiple_of(owner * chunk, chunk), chunk)

    def rows_of(device):
        return pl.ds(pl.multiple_of(device * local, local), local)

    barrier = pltpu.get_barrier_semaphore()
    for peer in mem_peers:
        pl.semaphore_signal(barrier, inc=1, device_id={"mem": peer}, device_id_type=MESH)
    for peer in space_peers:
        pl.semaphore_signal(barrier, inc=1, device_id={"space": peer}, device_id_type=MESH)
    pl.semaphore_wait(barrier, n_mem - 1 + n_space - 1)

    def spot(whole, slabs, piece, device):
        start, count = pieces[piece]
        if aligned:
            return whole.at[start : start + count, rows_of(device), :]
        return slabs.at[device, start : start + count]

    def outside(array, piece, owner):
        start, count = pieces[piece]
        return array.at[start : start + count, :, lanes_of(owner)]

    def inward(piece, peer, source):
        return pltpu.make_async_remote_copy(
            src_ref=outside(ensemble, piece, peer),
            dst_ref=spot(arrived, in_slabs, piece, source),
            send_sem=in_send.at[piece, peer],
            recv_sem=in_recv.at[piece, source],
            device_id={"mem": peer},
            device_id_type=MESH,
        )

    def inward_own(piece):
        return pltpu.make_async_copy(
            outside(ensemble, piece, me), spot(arrived, in_slabs, piece, me), own_in.at[piece]
        )

    def outward(piece, peer, owner):
        return pltpu.make_async_remote_copy(
            src_ref=spot(results, out_slabs, piece, peer),
            dst_ref=outside(analysis, piece, owner),
            send_sem=out_send.at[piece, peer],
            recv_sem=out_recv.at[piece, owner],
            device_id={"mem": peer},
            device_id_type=MESH,
        )

    def outward_own(piece):
        return pltpu.make_async_copy(
            spot(results, out_slabs, piece, me), outside(analysis, piece, me), own_out.at[piece]
        )

    owns = me < active
    for group in (beside, across):
        for piece in range(len(pieces)):
            for peer in group:
                when(partial_owners, peer < active, lambda: inward(piece, peer, me).start())
    for piece in range(len(pieces)):
        when(partial_owners, owns, lambda: inward_own(piece).start())
    loads = [
        pltpu.make_async_copy(source, target, small_sem.at[index])
        for index, (source, target) in enumerate(
            zip(smalls, (transform, obs_operator, obs_weight))
        )
    ]
    for load in loads:
        load.start()
    for load in loads:
        load.wait()

    eye = as_bf16(selector((members, members), lambda r, c: r == c))
    mixing_t = lax.dot_general(eye, transform[...], NT, preferred_element_type=jnp.float32)
    keep = 1.0 - jnp.sum(mixing_t, axis=1, keepdims=True)
    ones = jnp.ones((ROWS, members), jnp.float32)
    mixer = jnp.concatenate([mixing_t, ones], axis=0).astype(jnp.bfloat16)

    obs_rows = n_obs * ROWS
    obs_pick = as_bf16(selector((obs_rows, n_obs), lambda r, c: r // ROWS == c))
    for piece, (start, count) in enumerate(pieces):
        depth = count * ROWS
        place = as_bf16(selector((variables, depth), lambda r, c: r == c // ROWS + start))
        part = dot(obs_operator[...], place).astype(jnp.bfloat16)
        mask = selector((obs_rows, depth), lambda r, c: lax.rem(r, ROWS) == lax.rem(c, ROWS))
        full = jnp.where(mask, dot(obs_pick, part), 0.0)
        observer[piece, :, 0:depth] = full.astype(jnp.bfloat16)

    def mix(piece):
        start, count = pieces[piece]
        for variable in range(start, start + count):
            if not aligned:
                for device in range(n_mem):
                    rows = slice(device * local, (device + 1) * local)
                    arrived[variable, rows, :] = in_slabs[device, variable]
            mixed = dot(mixer, arrived[variable])
            mean = mixed[members : members + 1, :] / members
            value = (mixed[:members, :] + keep * mean).astype(jnp.bfloat16)
            if aligned:
                results[variable] = value
            else:
                for device in range(n_mem):
                    rows = slice(device * local, (device + 1) * local)
                    out_slabs[device, variable] = value[rows, :]

    def observe(piece):
        start, count = pieces[piece]
        depth = count * ROWS
        for block in range(blocks):
            at = slice(block * ROWS, (block + 1) * ROWS)
            states = arrived[start : start + count, at, :].reshape(depth, chunk)
            term = dot(observer[piece, :, 0:depth], states).reshape(n_obs, ROWS, chunk)
            if piece == 0:
                observed[:, at, :] = term
            else:
                observed[:, at, :] += term

    def form_gram():
        weights = obs_weight[:, lanes_of(me)]
        total = jnp.zeros((members, members), jnp.float32)
        for quantity in range(n_obs):
            values = observed[quantity]
            departures = values - jnp.sum(values, axis=0, keepdims=True) / members
            total += lax.dot_general(
                departures * weights[quantity : quantity + 1, :],
                departures,
                NT,
                precision=HIGHEST,
                preferred_element_type=jnp.float32,
            )
        gram[0:members, 0:members] = total
        gram[members : members + 8, :] = jnp.full((8, LANES), jnp.sum(weights), jnp.float32)

    gram[...] = jnp.zeros_like(gram)

    last = len(pieces) - 1

    def send_back(piece, group):
        for peer in group:
            outward(piece, peer, me).start()

    def work():
        for piece in range(last + 1):
            for peer in mem_peers:
                inward(piece, me, peer).wait_recv()
            inward_own(piece).wait()
            mix(piece)
            send_back(piece, beside)
            if piece < last:
                pl.when(central)(lambda: send_back(piece, across))
            outward_own(piece).start()
            observe(piece)
        form_gram()

    def finish_sends():
        for piece in range(last):
            pl.when(jnp.logical_not(central))(lambda: send_back(piece, across))
        send_back(last, across)

    when(partial_owners, owns, work)

    def exchange(source, slots, index, peers, axis, send, recv, between):
        slots[index] = source
        copies = [
            pltpu.make_async_remote_copy(
                src_ref=slots.at[index],
                dst_ref=slots.at[index],
                send_sem=send.at[peer],
                recv_sem=recv.at[index],
                device_id={axis: peer},
                device_id_type=MESH,
            )
            for peer in peers
        ]
        for copy in copies:
            copy.start()
        between()
        for peer in peers:
            pltpu.make_async_remote_copy(
                src_ref=slots.at[peer],
                dst_ref=slots.at[peer],
                send_sem=send.at[peer],
                recv_sem=recv.at[peer],
                device_id={axis: peer},
                device_id_type=MESH,
            ).wait_recv()
        total = slots[0]
        for slot in range(1, slots.shape[0]):
            total += slots[slot]
        for copy in copies:
            copy.wait_send()
        return total

    total = exchange(
        gram[...], by_space, here, space_peers, "space", space_send, space_recv, lambda: None
    )
    total = exchange(
        total, by_mem, me, mem_peers, "mem", mem_send, mem_recv,
        lambda: when(partial_owners, owns, finish_sends),
    )
    prior_gram = total[0:members, 0:members] / total[members : members + 1, 0:members]
    prior[...] = prior_gram
    carried = jnp.dot(
        mixing_t, prior_gram, precision=HIGHEST, preferred_element_type=jnp.float32
    )
    posterior[...] = jnp.dot(
        carried,
        transform[...].astype(jnp.float32),
        precision=HIGHEST,
        preferred_element_type=jnp.float32,
    )

    for piece in range(len(pieces)):
        for peer in mem_peers:
            when(partial_owners, peer < active, lambda: inward(piece, peer, me).wait_send())
            when(partial_owners, owns, lambda: outward(piece, peer, me).wait_send())
            when(partial_owners, peer < active, lambda: outward(piece, me, peer).wait_recv())
        when(partial_owners, owns, lambda: outward_own(piece).wait())


def hub_kernel(
    sizes, ensemble, transform_in, operator_in, weight_in, analysis, prior, posterior,
    transform, obs_operator, obs_weight, arrived, relay, results, observer, observed,
    gram, parts, summed, crossed, totals, sem, arrive, passing, ready,
):
    n_mem, n_space, pieces, local, members, variables, n_obs, half = sizes
    blocks = members // ROWS
    quarter = members // n_space
    me = lax.axis_index("mem")
    here = lax.axis_index("space")
    side = me // (n_mem // 2)
    is_hub = jnp.logical_or(me * 2 == n_mem, (me + 1) * 2 == n_mem)
    is_end = jnp.logical_not(is_hub)
    last_mem = n_mem - 1
    own_hub, far_hub = 1 + side, 2 - side
    own_end, far_end = last_mem * side, last_mem - last_mem * side
    space_peers = [lax.rem(here + step, n_space) for step in range(1, n_space)]
    order = range(len(pieces))

    def lanes_of(which):
        return pl.ds(pl.multiple_of(which * half, half), half)

    def rows_of(device):
        return pl.ds(pl.multiple_of(device * local, local), local)

    def quarter_of(device):
        return pl.ds(pl.multiple_of(device * quarter, quarter), quarter)

    def signal(sem, **device):
        pl.semaphore_signal(sem, inc=1, device_id=device, device_id_type=MESH)

    def remote(source, target, send, recv, **device):
        return pltpu.make_async_remote_copy(
            src_ref=source, dst_ref=target, send_sem=send, recv_sem=recv,
            device_id=device, device_id_type=MESH,
        )

    def span(piece):
        start, count = pieces[piece]
        return slice(start, start + count)

    def raw(piece, source, lanes_side):
        return remote(
            ensemble.at[span(piece), :, lanes_of(lanes_side)],
            arrived.at[span(piece), rows_of(source), :],
            sem.at[SENT], arrive.at[piece], mem=far_hub,
        )

    def forward(piece, source):
        return remote(
            relay.at[span(piece)], arrived.at[span(piece), rows_of(source), :],
            sem.at[SENT], arrive.at[piece], mem=far_hub,
        )

    def to_hub(piece):
        return remote(
            ensemble.at[span(piece), :, lanes_of(side)],
            arrived.at[span(piece), rows_of(own_end), :],
            sem.at[SENT], arrive.at[piece], mem=own_hub,
        )

    def to_relay(piece):
        return remote(
            ensemble.at[span(piece), :, lanes_of(1 - side)], relay.at[span(piece)],
            sem.at[SENT], passing.at[piece], mem=own_hub,
        )

    def own_raw(piece):
        return pltpu.make_async_copy(
            ensemble.at[span(piece), :, lanes_of(side)],
            arrived.at[span(piece), rows_of(me), :],
            arrive.at[piece],
        )

    def outward(block, piece, peer):
        rows = span(piece)
        return remote(
            results.at[rows, block * local : (block + 1) * local, :],
            analysis.at[rows, :, lanes_of(side)],
            sem.at[OUT], sem.at[FINAL], mem=peer,
        )

    def to_end():
        return remote(totals, totals, sem.at[LAST], sem.at[CROSS], mem=own_end)

    def landed(ref, semaphore):
        remote(ref, ref, semaphore, semaphore, mem=far_hub).wait_recv()

    def left(ref, semaphore):
        remote(ref, ref, semaphore, semaphore, mem=far_hub).wait_send()

    loads = [
        pltpu.make_async_copy(source, target, sem.at[index])
        for index, source, target in zip(
            (OUT, LAST, SMALL),
            (transform_in, operator_in, weight_in),
            (transform, obs_operator, obs_weight),
        )
    ]
    barrier = pltpu.get_barrier_semaphore()

    @pl.when(is_hub)
    def _():
        signal(barrier, mem=far_hub)
        pl.semaphore_wait(barrier, 1)
        for piece in range(LEAD):
            raw(piece, me, 1 - side).start()
        signal(barrier, mem=own_end)
        signal(barrier, mem=far_end)
        for piece in order:
            own_raw(piece).start()

    @pl.when(is_end)
    def _():
        for peer in space_peers:
            signal(barrier, space=peer)
        pl.semaphore_wait(barrier, 2 + n_space - 1)
        to_relay(0).start()
        for piece in order:
            if piece + 1 < len(pieces):
                to_relay(piece + 1).start()
            to_hub(piece).start()
        for peer in space_peers:
            signal(ready, space=peer)
        pl.semaphore_wait(ready, n_space - 1)
        signal(ready, mem=own_hub)
        signal(ready, mem=far_hub)

    for load in loads:
        load.start()
    for load in loads:
        load.wait()
    eye = as_bf16(selector((members, members), lambda r, c: r == c))
    mixing_t = lax.dot_general(eye, transform[...], NT, preferred_element_type=jnp.float32)

    def device_of(block):
        outer = jnp.where(block == 1, own_end, far_end)
        inner = jnp.where(block == 0, own_hub, far_hub)
        return jnp.where(jnp.logical_or(block == 0, block == 2), inner, outer)

    def work():
        placed = as_bf16(selector(
            (members, members), lambda r, c: c == device_of(r // local) * local + lax.rem(r, local)
        ))
        ordered = lax.dot_general(placed, transform[...], NT, preferred_element_type=jnp.float32)
        keep = 1.0 - jnp.sum(ordered, axis=1, keepdims=True)
        ones = jnp.ones((ROWS, members), jnp.float32)
        mixer = jnp.concatenate([ordered, ones], axis=0).astype(jnp.bfloat16)

        obs_rows = n_obs * ROWS
        obs_pick = as_bf16(selector((obs_rows, n_obs), lambda r, c: r // ROWS == c))
        for piece, (start, count) in enumerate(pieces):
            depth = count * ROWS
            place = as_bf16(selector((variables, depth), lambda r, c: r == c // ROWS + start))
            part = dot(obs_operator[...], place).astype(jnp.bfloat16)
            mask = selector((obs_rows, depth), lambda r, c: lax.rem(r, ROWS) == lax.rem(c, ROWS))
            full = jnp.where(mask, dot(obs_pick, part), 0.0)
            observer[piece, :, 0:depth] = full.astype(jnp.bfloat16)

        def feed(piece):
            landed(relay.at[span(piece)], passing.at[piece])
            forward(piece, own_end).start()
            if piece + LEAD < len(pieces):
                raw(piece + LEAD, me, 1 - side).start()

        def take(piece):
            landed(arrived.at[span(piece)], arrive.at[piece])

        def mix(piece):
            start, count = pieces[piece]

            def several(step, carry):
                for offset in range(2):
                    variable = start + step * 2 + offset
                    mixed = dot(mixer, arrived[variable])
                    mean = mixed[members : members + 1, :] / members
                    value = (mixed[:members, :] + keep * mean).astype(jnp.bfloat16)
                    analysis[variable, :, lanes_of(side)] = value[0:local, :]
                    results[variable] = value[local:, :]
                return carry

            lax.fori_loop(0, count // 2, several, 0)

        def observe(piece):
            start, count = pieces[piece]
            depth = count * ROWS
            def one(block, carry):
                at = pl.ds(pl.multiple_of(block * ROWS, ROWS), ROWS)
                states = arrived[start : start + count, at, :].reshape(depth, half)
                term = dot(observer[piece, :, 0:depth], states).reshape(n_obs, ROWS, half)
                if piece == 0:
                    observed[:, at, :] = term
                else:
                    observed[:, at, :] += term
                return carry

            lax.fori_loop(0, blocks, one, 0)

        def form_gram():
            def one(quantity, total):
                values = observed[quantity]
                departures = values - jnp.sum(values, axis=0, keepdims=True) / members
                weight = obs_weight[pl.ds(quantity, 1), lanes_of(side)]
                return total + lax.dot_general(
                    departures * weight,
                    departures,
                    NT,
                    precision=HIGHEST,
                    preferred_element_type=jnp.float32,
                )

            total = lax.fori_loop(0, n_obs, one, jnp.zeros((members, members), jnp.float32))
            gram[...] = jnp.full(gram.shape, jnp.sum(obs_weight[...]), jnp.float32)
            gram[:, 0:members] = total

        def to_part(peer):
            return remote(
                gram.at[quarter_of(peer)], parts.at[here],
                sem.at[SMALL], sem.at[PART], space=peer,
            )

        def to_total(peer):
            return remote(
                totals.at[quarter_of(here)], totals.at[quarter_of(here)],
                sem.at[LAST], sem.at[TOTAL], space=peer,
            )

        to_cross = remote(summed, crossed, sem.at[SMALL], sem.at[CROSS], mem=far_hub)
        others = (n_space - 1) * quarter
        steps = len(pieces)
        for piece in range(min(LEAD, steps)):
            feed(piece)
        fed = min(LEAD, steps)
        pl.semaphore_wait(ready, 2)
        behind = []
        for piece in order:
            take(piece)
            mix(piece)
            outward(0, piece, own_end).start()
            behind.append(piece)
            if fed < steps:
                feed(fed)
                fed += 1
            if fed == steps:
                for ahead in behind:
                    outward(2, ahead, far_end).start()
                behind = []
            observe(piece)
        outward(1, 0, far_hub).start()
        form_gram()
        for peer in space_peers:
            to_part(peer).start()
        parts[here] = gram[quarter_of(here), :]
        landed(parts.at[0 : n_space - 1], sem.at[PART])
        total = parts[0]
        for slot in range(1, n_space):
            total += parts[slot]
        upper = quarter // 2
        summed[:, 0:members] = total[0:upper, 0:members]
        summed[:, members : 2 * members] = total[upper:, 0:members]
        left(gram.at[0:others], sem.at[SMALL])
        to_cross.start()
        for piece in order[1:]:
            outward(1, piece, far_hub).start()
        to_cross.wait_recv()
        totals[quarter_of(here), members:] = total[:, members:]
        whole = summed[...] + crossed[...]
        for part in range(2):
            rows = pl.ds(pl.multiple_of(here * quarter + part * upper, upper), upper)
            totals[rows, 0:members] = whole[:, part * members : (part + 1) * members]
        to_cross.wait_send()
        for peer in space_peers:
            to_total(peer).start()
        landed(totals.at[0:others], sem.at[TOTAL])
        left(totals.at[0:others], sem.at[LAST])
        to_end().start()

    pl.when(is_hub)(work)

    @pl.when(is_end)
    def _():
        to_end().wait_recv()

    prior_gram = totals[:, 0:members] / totals[:, members : members + 1]
    prior[...] = prior_gram
    carried = jnp.dot(
        mixing_t, prior_gram, precision=HIGHEST, preferred_element_type=jnp.float32
    )
    posterior[...] = jnp.dot(
        carried,
        transform[...].astype(jnp.float32),
        precision=HIGHEST,
        preferred_element_type=jnp.float32,
    )

    left(ensemble, sem.at[SENT])

    @pl.when(is_hub)
    def _():
        to_end().wait_send()
        left(results, sem.at[OUT])
        landed(analysis.at[:, :, lanes_of(1 - side)], sem.at[FINAL])

    @pl.when(is_end)
    def _():
        landed(analysis, sem.at[FINAL])


def hub_call(n_mem, n_space, pieces, ensemble, transform, obs_operator, obs_weight):
    variables, local, cells = ensemble.shape
    members = transform.shape[0]
    n_obs = obs_operator.shape[0]
    half = cells // 2
    sizes = (n_mem, n_space, pieces, local, members, variables, n_obs, half)
    vmem = pl.BlockSpec(memory_space=pltpu.VMEM)
    any_space = pl.BlockSpec(memory_space=pl.ANY)
    dma = pltpu.SemaphoreType.DMA
    steps = len(pieces)
    quarter = members // n_space
    return pl.pallas_call(
        functools.partial(hub_kernel, sizes),
        out_shape=(
            pltpu.VMEM((variables, local, cells), jnp.bfloat16),
            pltpu.VMEM((members, members), jnp.float32),
            pltpu.VMEM((members, members), jnp.float32),
        ),
        in_specs=[any_space] * 4,
        out_specs=(vmem, vmem, vmem),
        scratch_shapes=[
            pltpu.VMEM(transform.shape, jnp.bfloat16),
            pltpu.VMEM(obs_operator.shape, jnp.bfloat16),
            pltpu.VMEM(obs_weight.shape, jnp.float32),
            pltpu.VMEM((variables, members, half), jnp.bfloat16),
            pltpu.VMEM((variables, local, half), jnp.bfloat16),
            pltpu.VMEM((variables, members - local, half), jnp.bfloat16),
            pltpu.VMEM((steps, n_obs * ROWS, PIECE * ROWS), jnp.bfloat16),
            pltpu.VMEM((n_obs, members, half), jnp.float32),
            pltpu.VMEM((members, LANES), jnp.float32),
            pltpu.VMEM((n_space, quarter, LANES), jnp.float32),
            pltpu.VMEM((quarter // 2, LANES), jnp.float32),
            pltpu.VMEM((quarter // 2, LANES), jnp.float32),
            pltpu.VMEM((members, LANES), jnp.float32),
            dma((CROSS + 1,)),
            dma((steps,)),
            dma((steps,)),
            pltpu.SemaphoreType.REGULAR,
        ],
        compiler_params=pltpu.CompilerParams(collective_id=0, has_side_effects=True),
        name="hub_exchange",
    )(ensemble, transform, obs_operator, obs_weight)


def store(*refs):
    count = len(refs) // 2
    sources, targets, sems = refs[:count], refs[count : 2 * count], refs[-1]
    copies = [
        pltpu.make_async_copy(source, target, sems.at[index])
        for index, (source, target) in enumerate(zip(sources, targets))
    ]
    for copy in copies:
        copy.start()
    for copy in copies:
        copy.wait()


def write_out(*arrays):
    return pl.pallas_call(
        store,
        out_shape=tuple(jax.ShapeDtypeStruct(a.shape, a.dtype) for a in arrays),
        in_specs=[pl.BlockSpec(memory_space=pl.ANY)] * len(arrays),
        out_specs=tuple([pl.BlockSpec(memory_space=pl.ANY)] * len(arrays)),
        scratch_shapes=[pltpu.SemaphoreType.DMA((len(arrays),))],
        compiler_params=pltpu.CompilerParams(vmem_limit_bytes=8 << 20),
        name="store_outputs",
    )(*arrays)


def per_device(n_mem, n_space, ensemble, transform, obs_operator, obs_weight):
    local, variables, cells = ensemble.shape
    members = transform.shape[0]
    n_obs = obs_operator.shape[0]
    active = min(n_mem, cells // LANES)
    chunk = cells // active
    pieces = tuple(
        (start, min(PIECE, variables - start)) for start in range(0, variables, PIECE)
    )
    if (
        n_mem == 4
        and local == ROWS
        and 2 * members == LANES
        and members % (16 * n_space) == 0
        and cells % (2 * LANES) == 0
    ):
        by_variable, prior, posterior = write_out(*hub_call(
            n_mem, n_space, pieces, jnp.transpose(ensemble, (1, 0, 2)), transform, obs_operator, obs_weight
        ))
        return jnp.transpose(by_variable, (1, 0, 2)), prior, posterior
    sizes = (n_mem, n_space, active, pieces, local, members, variables, n_obs, chunk)
    vmem = pl.BlockSpec(memory_space=pltpu.VMEM)
    any_space = pl.BlockSpec(memory_space=pl.ANY)
    gram_shape = (members + 8, LANES)
    slabs = (1, 1, ROWS, LANES) if local % ROWS == 0 else (n_mem, variables, local, chunk)
    dma = pltpu.SemaphoreType.DMA
    by_variable, prior, posterior = pl.pallas_call(
        functools.partial(line_kernel, sizes),
        out_shape=(
            pltpu.VMEM((variables, local, cells), jnp.bfloat16),
            pltpu.VMEM((members, members), jnp.float32),
            pltpu.VMEM((members, members), jnp.float32),
        ),
        in_specs=[any_space] * 4,
        out_specs=(vmem, vmem, vmem),
        scratch_shapes=[
            pltpu.VMEM(transform.shape, jnp.bfloat16),
            pltpu.VMEM(obs_operator.shape, jnp.bfloat16),
            pltpu.VMEM(obs_weight.shape, jnp.float32),
            dma((3,)),
            pltpu.VMEM((variables, members, chunk), jnp.bfloat16),
            pltpu.VMEM((variables, members, chunk), jnp.bfloat16),
            pltpu.VMEM((len(pieces), n_obs * ROWS, PIECE * ROWS), jnp.bfloat16),
            pltpu.VMEM((n_obs, members, chunk), jnp.float32),
            pltpu.VMEM(gram_shape, jnp.float32),
            pltpu.VMEM((n_space,) + gram_shape, jnp.float32),
            pltpu.VMEM((n_mem,) + gram_shape, jnp.float32),
            pltpu.VMEM(slabs, jnp.bfloat16),
            pltpu.VMEM(slabs, jnp.bfloat16),
            dma((len(pieces), n_mem)),
            dma((len(pieces), n_mem)),
            dma((len(pieces), n_mem)),
            dma((len(pieces), n_mem)),
            dma((len(pieces),)),
            dma((len(pieces),)),
            dma((n_space,)),
            dma((n_space,)),
            dma((n_mem,)),
            dma((n_mem,)),
        ],
        compiler_params=pltpu.CompilerParams(collective_id=0, has_side_effects=True),
        name="ensemble_exchange",
    )(jnp.transpose(ensemble, (1, 0, 2)), transform, obs_operator, obs_weight)
    by_variable, prior, posterior = write_out(by_variable, prior, posterior)
    return jnp.transpose(by_variable, (1, 0, 2)), prior, posterior


def solution(mesh):
    return jax.shard_map(
        functools.partial(per_device, mesh.shape["mem"], mesh.shape["space"]),
        mesh=mesh,
        in_specs=(
            P("mem", None, ("parts", "space")),
            P("parts", None),
            P(),
            P(None, ("parts", "space")),
        ),
        out_specs=(P("mem", None, ("parts", "space")), P("parts", None), P("parts", None)),
        check_vma=False,
    )
```
